32 devices in a mesh: groups: 2 (over y), ctx: 16 (over z, x, core).
Axes of the slice: x: 2, y: 2, z: 4, core: 2. Of those that a mesh axis runs over, the one named last changes fastest.
Arguments:
- prompt_query: bfloat16 [2048, 4096], P(('groups', 'ctx')), parts along dimension 0, may hold values from -6 to 6
- prompt_key: bfloat16 [2048, 512], P(('groups', 'ctx')), parts along dimension 0, may hold values from -6 to 6
- prompt_value: bfloat16 [2048, 512], P(('groups', 'ctx')), parts along dimension 0, may hold values from -6 to 6
- prefix_key_cache: bfloat16 [256, 512], P(('groups', 'ctx')), parts along dimension 0, may hold values from -6 to 6
- prefix_value_cache: bfloat16 [256, 512], P(('groups', 'ctx')), parts along dimension 0, may hold values from -6 to 6
- decoded_query: bfloat16 [8192], P('groups'), parts along dimension 0, may hold values from -6 to 6
- decoded_key: bfloat16 [1024], P('groups'), parts along dimension 0, may hold values from -6 to 6
- decoded_value: bfloat16 [1024], P('groups'), parts along dimension 0, may hold values from -6 to 6
- shard_counts: int32 [32, 2], P('groups'), parts along dimension 0, may hold values from 0 to 32, as said below
- block_offsets: int32 [32, 2], P('groups'), parts along dimension 0, may hold values from 0 to 992, as said below
Outputs:
- span_out: bfloat16 [2048, 4096], P(('groups', 'ctx')), parts along dimension 0
- next_out: bfloat16 [8192], P('groups'), parts along dimension 0
The draws below stay inside these ranges and needn't reach their ends.
There are 2 independent parts, one for each index of `groups`. The reference program is written for one: setup_inputs(seed, part) draws one part's arguments, and reference() takes and returns one part's arrays. A program takes and returns all parts, laid end to end along the dimension named above; each array names one. Nothing has to cross between parts.
Inputs may be any that keep to these rules, and one draw needn't show every extreme that they name: block_offsets[i, 0] = 32 * p_i and block_offsets[i, 1] = 32 * (31 - p_i) for a permutation p of 0 to 15. shard_counts[i, h] = min(32, max(0, L - block_offsets[i, h])) for one prompt length L with 512 < L <= 960.
All inputs are finite; a program needn't handle non-finite values.
Results may differ from the reference program's by a relative error of at most 0.0055.
Values may be sent and summed in bfloat16 or wider, within the bound.
A program may use at most 128 MiB of HBM per device.

```python
import jax
import jax.numpy as jnp
from jax import lax

QUERY_HEADS = 32
KEY_VALUE_HEADS = 4
HEAD_WIDTH = 128
HEADS_PER_GROUP = 8
T_DEV = 64
C_DEV = 8
HALF = 32
PROMPT_SLOTS = 1024
PREFIX_LENGTH = 128
N_CTX = 16


def flipped_signs(key):
    random_flip_bits = jax.random.randint(jax.random.fold_in(key, 11), (KEY_VALUE_HEADS, HEAD_WIDTH), 0, 2)
    return (2 * random_flip_bits - 1).astype(jnp.float32)


def draw_prompt_query(key, part):
    value_matrix = jax.random.truncated_normal(jax.random.fold_in(key, 1), -6.0, 6.0, (PROMPT_SLOTS, QUERY_HEADS * HEAD_WIDTH), jnp.float32)
    random_sign_rows = jnp.repeat(flipped_signs(key), QUERY_HEADS // KEY_VALUE_HEADS, axis=0).reshape(QUERY_HEADS * HEAD_WIDTH)
    chosen = jax.random.randint(jax.random.fold_in(key, 2), (PROMPT_SLOTS,), 0, 32)
    levels = jax.random.randint(jax.random.fold_in(key, 3), (PROMPT_SLOTS,), 3, 7).astype(jnp.float32)
    value_matrix = jnp.where((chosen == 0)[:, None], levels[:, None] * random_sign_rows[None, :], value_matrix)
    return value_matrix.astype(jnp.bfloat16)


def draw_prefix_key_cache(key, part):
    value_matrix = jax.random.truncated_normal(jax.random.fold_in(key, 4), -6.0, 6.0, (PREFIX_LENGTH, KEY_VALUE_HEADS * HEAD_WIDTH), jnp.float32)
    random_sign_rows = flipped_signs(key).reshape(KEY_VALUE_HEADS * HEAD_WIDTH)
    hot_first = C_DEV + jax.random.randint(jax.random.fold_in(key, 5), (), 0, C_DEV)
    hot_second = C_DEV * (N_CTX // 2) + jax.random.randint(jax.random.fold_in(key, 6), (), 0, C_DEV)
    row_ids = jnp.arange(PREFIX_LENGTH)
    value_matrix = jnp.where((row_ids == hot_first)[:, None], 5.0 * random_sign_rows[None, :], value_matrix)
    value_matrix = jnp.where((row_ids == hot_second)[:, None], 5.0625 * random_sign_rows[None, :], value_matrix)
    return value_matrix.astype(jnp.bfloat16)


def decode_pair(key):
    random_sign_rows = flipped_signs(key)
    single_query_row = 4.0 * jnp.repeat(random_sign_rows, QUERY_HEADS // KEY_VALUE_HEADS, axis=0).reshape(QUERY_HEADS * HEAD_WIDTH)
    single_key_row = 5.0625 * random_sign_rows.reshape(KEY_VALUE_HEADS * HEAD_WIDTH)
    return (single_query_row, single_key_row)


def draw_decoded_query(key, part):
    return decode_pair(key)[0].astype(jnp.bfloat16)


def draw_decoded_key(key, part):
    return decode_pair(key)[1].astype(jnp.bfloat16)


def span_layout(key):
    ordering = jax.random.permutation(jax.random.fold_in(key, 21), N_CTX)
    starts = jnp.stack([ordering * HALF, (2 * N_CTX - 1 - ordering) * HALF], axis=1)
    prompt_len = jax.random.randint(jax.random.fold_in(key, 22), (), PROMPT_SLOTS // 2 + 1, PROMPT_SLOTS - T_DEV + 1)
    counts = jnp.clip(prompt_len - starts, 0, HALF)
    return (starts.astype(jnp.int32), counts.astype(jnp.int32))


def draw_block_offsets(key, part):
    return span_layout(key)[0]


def draw_shard_counts(key, part):
    return span_layout(key)[1]


def shard_levels(rng, extent, split, least, high):
    level, own = 1.0, jax.random.fold_in(rng, 6)
    for dim, blocks in split:
        draws = jnp.exp(jax.random.uniform(jax.random.fold_in(own, dim), (blocks,), jnp.float32, least / len(split), high / len(split)))
        level = level * jnp.repeat(draws, extent[dim] // blocks).reshape([-1 if axis == dim else 1 for axis in range(len(extent))])
    return level


def gaussian(own_key, dims, spread, limit, split=(), kind=jnp.bfloat16):
    gain = shard_levels(own_key, dims, split, -0.22, 0.18) if split else 1.0
    result = jax.random.normal(own_key, dims, jnp.float32) * spread * gain
    return jnp.minimum(jnp.maximum(result, -limit), limit).astype(kind)


def setup_inputs(seed: int = 0, part: int = 0) -> dict:
    arg_keys = jax.random.split(jax.random.key(seed), 11)
    own_keys = jax.random.split(jax.random.fold_in(arg_keys[10], part), 11)
    prompt_query = draw_prompt_query(jax.random.fold_in(jax.random.fold_in(arg_keys[10], part), 71), part)
    prompt_key = gaussian(own_keys[1], (PROMPT_SLOTS, KEY_VALUE_HEADS * HEAD_WIDTH), 1.0, 6.0, ((0, 16),))
    prompt_value = gaussian(own_keys[2], (PROMPT_SLOTS, KEY_VALUE_HEADS * HEAD_WIDTH), 1.0, 6.0, ((0, 16),))
    prefix_key_cache = draw_prefix_key_cache(jax.random.fold_in(jax.random.fold_in(arg_keys[10], part), 71), part)
    prefix_value_cache = gaussian(own_keys[4], (PREFIX_LENGTH, KEY_VALUE_HEADS * HEAD_WIDTH), 1.0, 6.0, ((0, 16),))
    decoded_query = draw_decoded_query(jax.random.fold_in(jax.random.fold_in(arg_keys[10], part), 71), part)
    decoded_key = draw_decoded_key(jax.random.fold_in(jax.random.fold_in(arg_keys[10], part), 71), part)
    decoded_value = gaussian(own_keys[7], (KEY_VALUE_HEADS * HEAD_WIDTH,), 1.0, 6.0)
    shard_counts = draw_shard_counts(jax.random.fold_in(jax.random.fold_in(arg_keys[10], part), 71), part)
    block_offsets = draw_block_offsets(jax.random.fold_in(jax.random.fold_in(arg_keys[10], part), 71), part)
    return dict(prompt_query=prompt_query, prompt_key=prompt_key, prompt_value=prompt_value, prefix_key_cache=prefix_key_cache, prefix_value_cache=prefix_value_cache, decoded_query=decoded_query, decoded_key=decoded_key, decoded_value=decoded_value, shard_counts=shard_counts, block_offsets=block_offsets)


def slot_layout(shard_counts, block_offsets):
    slot_ids = jnp.arange(PROMPT_SLOTS, dtype=jnp.int32)
    shard_ids = slot_ids // T_DEV
    within = slot_ids % T_DEV
    piece_ids = within // HALF
    offset_in = within % HALF
    position = PREFIX_LENGTH + block_offsets[shard_ids, piece_ids] + offset_in
    is_live = offset_in < shard_counts[shard_ids, piece_ids]
    return position.astype(jnp.int32), is_live


def reference(prompt_query, prompt_key, prompt_value, prefix_key_cache, prefix_value_cache, decoded_query, decoded_key, decoded_value, shard_counts, block_offsets):
    logit_scale = HEAD_WIDTH ** -0.5
    position, is_live = slot_layout(shard_counts, block_offsets)
    key_pos = jnp.concatenate([jnp.arange(PREFIX_LENGTH, dtype=jnp.int32), position])
    key_live = jnp.concatenate([jnp.ones((PREFIX_LENGTH,), dtype=bool), is_live])
    head_key_rows = jnp.concatenate([prefix_key_cache, prompt_key], 0).astype(jnp.float32).reshape(-1, KEY_VALUE_HEADS, HEAD_WIDTH)
    head_value_rows = jnp.concatenate([prefix_value_cache, prompt_value], 0).astype(jnp.float32).reshape(-1, KEY_VALUE_HEADS, HEAD_WIDTH)
    prompt_block_rows = 128 if PROMPT_SLOTS % 128 == 0 else PROMPT_SLOTS

    def one_block(block_item):
        query_rows, query_pos, query_live = block_item
        query_head_list = query_rows.astype(jnp.float32).reshape(prompt_block_rows, KEY_VALUE_HEADS, HEADS_PER_GROUP, HEAD_WIDTH)
        scores = jnp.einsum("tgqd,rgd->tgqr", query_head_list, head_key_rows) * logit_scale
        visible = key_live[None, :] & (key_pos[None, :] <= query_pos[:, None])
        scores = jnp.where(visible[:, None, None, :], scores, -jnp.inf)
        peaks = jnp.max(scores, axis=-1, keepdims=True)
        weights = jnp.exp(scores - peaks)
        totals = jnp.sum(weights, axis=-1)
        rounded = lax.optimization_barrier(weights.astype(jnp.bfloat16)).astype(jnp.float32)
        value_mixture = jnp.einsum("tgqr,rgd->tgqd", rounded, head_value_rows) / totals[..., None]
        value_mixture = jnp.where(query_live[:, None, None, None], value_mixture, 0.0)
        return value_mixture.reshape(prompt_block_rows, QUERY_HEADS * HEAD_WIDTH).astype(jnp.bfloat16)

    outputs = lax.map(one_block, (prompt_query.reshape(PROMPT_SLOTS // prompt_block_rows, prompt_block_rows, QUERY_HEADS * HEAD_WIDTH), position.reshape(-1, prompt_block_rows), is_live.reshape(-1, prompt_block_rows)))
    span_out = outputs.reshape(PROMPT_SLOTS, QUERY_HEADS * HEAD_WIDTH)

    decoded_query_row = decoded_query.astype(jnp.float32).reshape(KEY_VALUE_HEADS, HEADS_PER_GROUP, HEAD_WIDTH)
    next_scores = jnp.einsum("gqd,rgd->gqr", decoded_query_row, head_key_rows) * logit_scale
    next_scores = jnp.where(key_live[None, None, :], next_scores, -jnp.inf)
    self_score = jnp.einsum("sop,sp->so", decoded_query_row, decoded_key.astype(jnp.float32).reshape(KEY_VALUE_HEADS, HEAD_WIDTH)) * logit_scale
    peaks = jnp.maximum(jnp.max(next_scores, axis=-1), self_score)
    next_weights = jnp.exp(next_scores - peaks[..., None])
    self_weight = jnp.exp(self_score - peaks)
    totals = jnp.sum(next_weights, axis=-1) + self_weight
    rounded = lax.optimization_barrier(next_weights.astype(jnp.bfloat16)).astype(jnp.float32)
    value_mixture = jnp.einsum("gqr,rgd->gqd", rounded, head_value_rows)
    value_mixture = value_mixture + self_weight[..., None] * decoded_value.astype(jnp.float32).reshape(KEY_VALUE_HEADS, 1, HEAD_WIDTH)
    next_out = (value_mixture / totals[..., None]).reshape(QUERY_HEADS * HEAD_WIDTH).astype(jnp.bfloat16)
    return (span_out, next_out)
```

```python
import functools

import jax
import jax.numpy as jnp
from jax import lax
from jax.experimental import pallas as pl
from jax.experimental.pallas import tpu as pltpu
from jax.sharding import PartitionSpec as P

HEAD_WIDTH = 128
PIECES = 2
CHUNK = 4
LOG2E = 1.4426950408889634
FILL = -1e30
FAR = 1 << 29


class Body:
    def __init__(self, n, q, dq, dk, dv, counts, offsets, kv, out, nxt, peak, acc):
        self.n, self.q, self.dq, self.dk, self.dv = n, q, dq, dk, dv
        self.counts, self.offsets, self.kv, self.out, self.nxt = counts, offsets, kv, out, nxt
        self.peak, self.acc = peak, acc
        self.rows = q.shape[0]
        self.half = self.rows // 2
        self.prior = (kv.shape[2] - 2 * self.rows) // 2
        self.groups = dk.shape[0]
        self.per_piece = self.groups // PIECES
        self.per_group = q.shape[1] // HEAD_WIDTH // self.groups
        self.tall = self.per_group * self.rows
        self.total = self.tall + self.per_piece * self.per_group
        self.rate = HEAD_WIDTH**-0.5 * LOG2E

    def init(self):
        self.peak[...] = jnp.full(self.peak.shape, FILL, jnp.float32)
        self.acc[...] = jnp.zeros(self.acc.shape, jnp.float32)

    def query_positions(self, me):
        r = lax.broadcasted_iota(jnp.int32, (self.rows, 1), 0)
        second = r >= self.half
        offset = jnp.where(second, r - self.half, r)
        position = offset + jnp.where(second, self.offsets[1, me], self.offsets[0, me])
        live = offset < jnp.where(second, self.counts[1, me], self.counts[0, me])
        return position, live

    def bias(self, me, first):
        width = CHUNK * self.rows
        lane = lax.broadcasted_iota(jnp.int32, (1, width), 1)
        piece = lane // self.half
        offset = lane % self.half
        start = jnp.zeros((1, width), jnp.int32)
        count = jnp.zeros((1, width), jnp.int32)
        for i in range(CHUNK):
            for h in range(2):
                here = piece == 2 * i + h
                start = jnp.where(here, self.offsets[h, first + i], start)
                count = jnp.where(here, self.counts[h, first + i], count)
        position = jnp.where(offset < count, start + offset, FAR)
        own, _ = self.query_positions(me)
        span = jnp.where(position <= own, 0.0, FILL).astype(jnp.float32)
        step = jnp.where(position < FAR, 0.0, FILL).astype(jnp.float32)
        return span, step

    def queries(self, g):
        base = g * self.per_group
        parts = [
            self.q[:, (base + h) * HEAD_WIDTH : (base + h + 1) * HEAD_WIDTH]
            for h in range(self.per_group)
        ]
        piece_rows = self.per_piece * self.per_group
        top = (g // self.per_piece) * piece_rows
        parts.append(self.dq[top : top + piece_rows, :])
        return jnp.concatenate(parts, axis=0)

    def chunk_rows(self, g, first, start):
        j = g % self.per_piece
        block = self.kv[
            g // self.per_piece,
            pl.ds(first, CHUNK),
            start : start + self.rows,
            j * HEAD_WIDTH : (j + 1) * HEAD_WIDTH,
        ]
        return block.reshape(CHUNK * self.rows, HEAD_WIDTH)

    def prefix_rows(self, g, first, devices):
        j = g % self.per_piece
        block = self.kv[
            g // self.per_piece,
            pl.ds(first, devices),
            2 * self.rows :,
            j * HEAD_WIDTH : (j + 1) * HEAD_WIDTH,
        ].astype(jnp.float32)
        flat = (devices * self.prior, HEAD_WIDTH)
        keys = block[:, : self.prior].reshape(flat).astype(jnp.bfloat16)
        values = block[:, self.prior :].reshape(flat).astype(jnp.bfloat16)
        return keys, values

    def update(self, g, keys, values, masks):
        scores = lax.dot_general(
            self.queries(g), keys, (((1,), (1,)), ((), ())), preferred_element_type=jnp.float32
        )
        if masks is not None:
            span, step = masks
            width = span.shape[1]
            extra = scores.shape[1] - width
            if extra:
                span = jnp.concatenate([span, jnp.zeros((span.shape[0], extra), jnp.float32)], 1)
                step = jnp.concatenate([step, jnp.zeros((1, extra), jnp.float32)], 1)
            low = jnp.broadcast_to(step, (self.total - self.tall, step.shape[1]))
            scores = scores + jnp.concatenate([span] * self.per_group + [low], 0)
        old = self.peak[g]
        new = jnp.maximum(old, jnp.max(scores, axis=1, keepdims=True))
        weights = jnp.exp2((scores - new[:, :1]) * self.rate).astype(jnp.bfloat16)
        wide = jnp.concatenate([values, jnp.ones(values.shape, jnp.bfloat16)], 1)
        summed = jnp.dot(weights, wide, preferred_element_type=jnp.float32)
        scale = jnp.exp2((old - new) * self.rate)
        self.acc[g] = self.acc[g] * jnp.concatenate([scale, scale], 1) + summed
        self.peak[g] = new

    def chunk(self, g, first, masks, prefix):
        keys = self.chunk_rows(g, first, 0)
        values = self.chunk_rows(g, first, self.rows)
        if prefix:
            more_keys, more_values = self.prefix_rows(g, 0, self.n)
            keys = jnp.concatenate([keys, more_keys], 0)
            values = jnp.concatenate([values, more_values], 0)
        self.update(g, keys, values, masks)

    def finish(self, g, me):
        _, live = self.query_positions(me)
        base = g * self.per_group
        for h in range(self.per_group):
            part = self.acc[g, h * self.rows : (h + 1) * self.rows, :]
            result = part[:, :HEAD_WIDTH] / part[:, HEAD_WIDTH:]
            result = jnp.where(live, result, 0.0).astype(jnp.bfloat16)
            self.out[:, (base + h) * HEAD_WIDTH : (base + h + 1) * HEAD_WIDTH] = result

    def finish_step(self, piece):
        results = []
        for j in range(self.per_piece):
            g = piece * self.per_piece + j
            top = self.tall + j * self.per_group
            part = self.acc[g, top : top + self.per_group, :]
            old = self.peak[g, top : top + self.per_group, :]
            rows = self.per_piece * self.per_group
            query = self.dq[piece * rows : (piece + 1) * rows, :].astype(jnp.float32)
            query = query[j * self.per_group : (j + 1) * self.per_group]
            key = self.dk[g : g + 1, :].astype(jnp.float32)
            value = self.dv[g : g + 1, :].astype(jnp.float32)
            score = jnp.sum(query * key, axis=1, keepdims=True)
            new = jnp.maximum(old, score)
            keep = jnp.exp2((old - new) * self.rate)
            own = jnp.exp2((score - new) * self.rate)
            top_sum = keep * part[:, :HEAD_WIDTH] + own * value
            results.append(top_sum / (keep * part[:, HEAD_WIDTH:] + own))
        rows = self.per_piece * self.per_group
        self.nxt[piece * rows : (piece + 1) * rows, :] = jnp.concatenate(results, 0).astype(
            jnp.bfloat16
        )


def ring_kernel(
    n,
    counts,
    offsets,
    pk,
    pv,
    ck,
    cv,
    q_hbm,
    dq,
    dk,
    dv,
    out,
    nxt,
    kv,
    q,
    peak,
    acc,
    sends,
    recvs,
    local,
):
    me = lax.axis_index("ctx")
    lines = n // CHUNK
    z, x, c = me // CHUNK, (me // 2) % 2, me % 2
    last = lines - 1
    half = kv.shape[3]
    own_copies = []
    for p in range(PIECES):
        top = 0
        for i, source in enumerate((pk, pv, ck, cv)):
            rows = source.shape[0]
            own_copies.append(
                pltpu.make_async_copy(
                    source.at[:, p * half : (p + 1) * half],
                    kv.at[p, me, top : top + rows],
                    local.at[4 * p + i],
                )
            )
            top += rows
    for d in own_copies:
        d.start()
    q_copy = pltpu.make_async_copy(q_hbm, q, local.at[8])
    q_copy.start()
    to_x = z * CHUNK + (1 - x) * 2 + c
    to_core = z * CHUNK + x * 2 + (1 - c)
    targets = (me + CHUNK, me - CHUNK, to_x, to_core)

    barrier = pltpu.get_barrier_semaphore()

    def greet(target):
        pl.semaphore_signal(
            barrier, inc=1, device_id={"ctx": target}, device_id_type=pl.DeviceIdType.MESH
        )

    greet(to_x)
    greet(to_core)

    @pl.when(z < last)
    def _():
        greet(me + CHUNK)

    @pl.when(z > 0)
    def _():
        greet(me - CHUNK)

    inner = jnp.where((z > 0) & (z < last), 1, 0).astype(jnp.int32)
    pl.semaphore_wait(barrier, 3 + inner)

    def copy(way, source, p):
        return pltpu.make_async_remote_copy(
            src_ref=kv.at[p, source],
            dst_ref=kv.at[p, source],
            send_sem=sends.at[way, source, p],
            recv_sem=recvs.at[source, p],
            device_id={"ctx": targets[way]},
            device_id_type=pl.DeviceIdType.MESH,
        )

    def column(line):
        return line * CHUNK + x * 2 + c

    def spread(line, p, act):
        @pl.when((line <= z) & (z < last))
        def _():
            act(copy(0, column(line), p))

        @pl.when((line >= z) & (z > 0))
        def _():
            act(copy(1, column(line), p))

        act(copy(2, column(line), p))
        act(copy(3, column(line), p))

    def other(line):
        return line * CHUNK + (1 - x) * 2 + c

    def start(d):
        d.start()

    near = jnp.minimum(z, last - z)
    lower = z < lines // 2
    order = []
    for s in range(lines):
        base = s if s >= 2 else (near if s == 0 else 1 - near)
        order.append(jnp.where(lower, base, last - base))

    for p in range(PIECES):
        for d in own_copies[4 * p : 4 * p + 4]:
            d.wait()
        spread(z, p, start)

    body = Body(n, q, dq, dk, dv, counts, offsets, kv, out, nxt, peak, acc)
    body.init()

    def from_column(s, p):
        copy(2, column(order[s]), p).wait_recv()
        spread(order[s], p, start)

    def from_x(s, p):
        copy(3, other(order[s]), p).wait_recv()
        copy(3, other(order[s]), p).start()

    def from_core(s, p):
        for side in range(2):
            copy(2, order[s] * CHUNK + side * 2 + (1 - c), p).wait_recv()

    for p in range(PIECES):
        from_column(1, p)
        from_x(0, p)
    q_copy.wait()
    for s in range(lines):
        final = s == lines - 1
        masks = body.bias(me, order[s] * CHUNK)
        for p in range(PIECES):
            if s + 2 < lines:
                from_column(s + 2, p)
            from_core(s, p)
            for j in range(body.per_piece):
                body.chunk(p * body.per_piece + j, order[s] * CHUNK, masks, final)
            if s + 1 < lines:
                from_x(s + 1, p)
            if final:
                for j in range(body.per_piece):
                    body.finish(p * body.per_piece + j, me)
                body.finish_step(p)
    for s in range(lines):
        for p in range(PIECES):
            spread(order[s], p, lambda d: d.wait_send())
            copy(3, other(order[s]), p).wait_send()


def local_kernel(n, counts, offsets, kv, q, dq, dk, dv, out, nxt, peak, acc):
    me = lax.axis_index("ctx")
    body = Body(n, q, dq, dk, dv, counts, offsets, kv, out, nxt, peak, acc)
    body.init()
    devices = HEAD_WIDTH // body.prior
    for g in range(body.groups):

        def step(i, carry):
            body.chunk(g, i * CHUNK, body.bias(me, i * CHUNK), False)
            return carry

        def prefix_step(i, carry):
            keys, values = body.prefix_rows(g, i * devices, devices)
            body.update(g, keys, values, None)
            return carry

        lax.fori_loop(0, n // CHUNK, step, 0)
        lax.fori_loop(0, n // devices, prefix_step, 0)
        body.finish(g, me)
    for p in range(PIECES):
        body.finish_step(p)


def body_fn(
    prompt_query,
    prompt_key,
    prompt_value,
    prefix_key_cache,
    prefix_value_cache,
    decoded_query,
    decoded_key,
    decoded_value,
    shard_counts,
    block_offsets,
):
    n = lax.axis_size("ctx")
    rows = prompt_query.shape[0]
    groups = prompt_key.shape[1] // HEAD_WIDTH
    heads = prompt_query.shape[1] // HEAD_WIDTH
    blocks = (prompt_key, prompt_value, prefix_key_cache, prefix_value_cache)
    tables = (shard_counts.T, block_offsets.T)
    half = prompt_key.shape[1] // PIECES
    height = sum(b.shape[0] for b in blocks)
    dq = decoded_query.reshape(heads, HEAD_WIDTH)
    dk = decoded_key.reshape(groups, HEAD_WIDTH)
    dv = decoded_value.reshape(groups, HEAD_WIDTH)
    total = heads // groups * rows + heads // PIECES
    smem = pl.BlockSpec(memory_space=pltpu.SMEM)
    vmem = pl.BlockSpec(memory_space=pltpu.VMEM)
    hbm = pl.BlockSpec(memory_space=pl.ANY)
    out_shape = (
        jax.ShapeDtypeStruct(prompt_query.shape, jnp.bfloat16),
        jax.ShapeDtypeStruct((heads, HEAD_WIDTH), jnp.bfloat16),
    )
    state = [
        pltpu.VMEM((groups, total, HEAD_WIDTH), jnp.float32),
        pltpu.VMEM((groups, total, 2 * HEAD_WIDTH), jnp.float32),
    ]
    if n == 4 * CHUNK:
        span, nxt = pl.pallas_call(
            functools.partial(ring_kernel, n),
            out_shape=out_shape,
            in_specs=[smem, smem, hbm, hbm, hbm, hbm, hbm, vmem, vmem, vmem],
            out_specs=(vmem, vmem),
            scratch_shapes=[
                pltpu.VMEM((PIECES, n, height, half), jnp.bfloat16),
                pltpu.VMEM(prompt_query.shape, jnp.bfloat16),
                *state,
                pltpu.SemaphoreType.DMA((4, n, PIECES)),
                pltpu.SemaphoreType.DMA((n, PIECES)),
                pltpu.SemaphoreType.DMA((9,)),
            ],
            compiler_params=pltpu.CompilerParams(
                collective_id=0, has_side_effects=True, vmem_limit_bytes=48 * 1024 * 1024
            ),
        )(*tables, *blocks, prompt_query, dq, dk, dv)
    else:
        joined = jnp.concatenate(blocks, axis=0)
        joined = jnp.stack([joined[:, p * half : (p + 1) * half] for p in range(PIECES)], 0)
        gathered = lax.all_gather(joined, "ctx", axis=1)
        span, nxt = pl.pallas_call(
            functools.partial(local_kernel, n),
            out_shape=out_shape,
            in_specs=[smem, smem, vmem, vmem, vmem, vmem, vmem],
            out_specs=(vmem, vmem),
            scratch_shapes=state,
            compiler_params=pltpu.CompilerParams(vmem_limit_bytes=56 * 1024 * 1024),
        )(*tables, gathered, prompt_query, dq, dk, dv)
    return span, nxt.reshape(heads * HEAD_WIDTH)


def solution(mesh):
    both = P(("groups", "ctx"), None)
    in_specs = (
        both,
        both,
        both,
        both,
        both,
        P("groups"),
        P("groups"),
        P("groups"),
        P("groups", None),
        P("groups", None),
    )
    out_specs = (both, P("groups"))
    return jax.shard_map(
        body_fn, mesh=mesh, in_specs=in_specs, out_specs=out_specs, check_vma=False
    )
```

```python
import functools

import jax
import jax.numpy as jnp
from jax import lax
from jax.experimental import pallas as pl
from jax.experimental.pallas import tpu as pltpu
from jax.sharding import PartitionSpec as P

HEAD_WIDTH = 128
PIECES = 2
CHUNK = 4
LOG2E = 1.4426950408889634
FILL = -1e30
FAR = 1 << 29


class Body:
    def __init__(self, n, q, dq, dk, dv, counts, offsets, kv, out, nxt, peak, acc):
        self.n, self.q, self.dq, self.dk, self.dv = n, q, dq, dk, dv
        self.counts, self.offsets, self.kv, self.out, self.nxt = counts, offsets, kv, out, nxt
        self.peak, self.acc = peak, acc
        self.rows = q.shape[0]
        self.half = self.rows // 2
        self.prior = (kv.shape[2] - 2 * self.rows) // 2
        self.groups = dk.shape[0]
        self.per_piece = self.groups // PIECES
        self.per_group = q.shape[1] // HEAD_WIDTH // self.groups
        self.tall = self.per_group * self.rows
        self.total = self.tall + self.per_piece * self.per_group
        self.rate = HEAD_WIDTH**-0.5 * LOG2E

    def init(self):
        self.peak[...] = jnp.full(self.peak.shape, FILL, jnp.float32)
        self.acc[...] = jnp.zeros(self.acc.shape, jnp.float32)

    def query_positions(self, me):
        r = lax.broadcasted_iota(jnp.int32, (self.rows, 1), 0)
        second = r >= self.half
        offset = jnp.where(second, r - self.half, r)
        position = offset + jnp.where(second, self.offsets[1, me], self.offsets[0, me])
        live = offset < jnp.where(second, self.counts[1, me], self.counts[0, me])
        return position, live

    def bias(self, me, first):
        width = CHUNK * self.rows
        lane = lax.broadcasted_iota(jnp.int32, (1, width), 1)
        piece = lane // self.half
        offset = lane % self.half
        start = jnp.zeros((1, width), jnp.int32)
        count = jnp.zeros((1, width), jnp.int32)
        for i in range(CHUNK):
            for h in range(2):
                here = piece == 2 * i + h
                start = jnp.where(here, self.offsets[h, first + i], start)
                count = jnp.where(here, self.counts[h, first + i], count)
        position = jnp.where(offset < count, start + offset, FAR)
        own, _ = self.query_positions(me)
        span = jnp.where(position <= own, 0.0, FILL).astype(jnp.float32)
        step = jnp.where(position < FAR, 0.0, FILL).astype(jnp.float32)
        return span, step

    def queries(self, g):
        base = g * self.per_group
        parts = [
            self.q[:, (base + h) * HEAD_WIDTH : (base + h + 1) * HEAD_WIDTH]
            for h in range(self.per_group)
        ]
        piece_rows = self.per_piece * self.per_group
        top = (g // self.per_piece) * piece_rows
        parts.append(self.dq[top : top + piece_rows, :])
        return jnp.concatenate(parts, axis=0)

    def chunk_rows(self, g, first, start):
        j = g % self.per_piece
        block = self.kv[
            g // self.per_piece,
            pl.ds(first, CHUNK),
            start : start + self.rows,
            j * HEAD_WIDTH : (j + 1) * HEAD_WIDTH,
        ]
        return block.reshape(CHUNK * self.rows, HEAD_WIDTH)

    def prefix_rows(self, g, first, devices):
        j = g % self.per_piece
        block = self.kv[
            g // self.per_piece,
            pl.ds(first, devices),
            2 * self.rows :,
            j * HEAD_WIDTH : (j + 1) * HEAD_WIDTH,
        ].astype(jnp.float32)
        flat = (devices * self.prior, HEAD_WIDTH)
        keys = block[:, : self.prior].reshape(flat).astype(jnp.bfloat16)
        values = block[:, self.prior :].reshape(flat).astype(jnp.bfloat16)
        return keys, values

    def update(self, g, keys, values, masks):
        scores = lax.dot_general(
            self.queries(g), keys, (((1,), (1,)), ((), ())), preferred_element_type=jnp.float32
        )
        if masks is not None:
            span, step = masks
            width = span.shape[1]
            extra = scores.shape[1] - width
            if extra:
                span = jnp.concatenate([span, jnp.zeros((span.shape[0], extra), jnp.float32)], 1)
                step = jnp.concatenate([step, jnp.zeros((1, extra), jnp.float32)], 1)
            low = jnp.broadcast_to(step, (self.total - self.tall, step.shape[1]))
            scores = scores + jnp.concatenate([span] * self.per_group + [low], 0)
        old = self.peak[g]
        new = jnp.maximum(old, jnp.max(scores, axis=1, keepdims=True))
        weights = jnp.exp2((scores - new[:, :1]) * self.rate).astype(jnp.bfloat16)
        wide = jnp.concatenate([values, jnp.ones(values.shape, jnp.bfloat16)], 1)
        summed = jnp.dot(weights, wide, preferred_element_type=jnp.float32)
        scale = jnp.exp2((old - new) * self.rate)
        self.acc[g] = self.acc[g] * jnp.concatenate([scale, scale], 1) + summed
        self.peak[g] = new

    def chunk(self, g, first, masks, prefix):
        keys = self.chunk_rows(g, first, 0)
        values = self.chunk_rows(g, first, self.rows)
        if prefix:
            more_keys, more_values = self.prefix_rows(g, 0, self.n)
            keys = jnp.concatenate([keys, more_keys], 0)
            values = jnp.concatenate([values, more_values], 0)
        self.update(g, keys, values, masks)

    def finish(self, g, me):
        _, live = self.query_positions(me)
        base = g * self.per_group
        for h in range(self.per_group):
            part = self.acc[g, h * self.rows : (h + 1) * self.rows, :]
            result = part[:, :HEAD_WIDTH] / part[:, HEAD_WIDTH:]
            result = jnp.where(live, result, 0.0).astype(jnp.bfloat16)
            self.out[:, (base + h) * HEAD_WIDTH : (base + h + 1) * HEAD_WIDTH] = result

    def finish_step(self, piece):
        results = []
        for j in range(self.per_piece):
            g = piece * self.per_piece + j
            top = self.tall + j * self.per_group
            part = self.acc[g, top : top + self.per_group, :]
            old = self.peak[g, top : top + self.per_group, :]
            rows = self.per_piece * self.per_group
            query = self.dq[piece * rows : (piece + 1) * rows, :].astype(jnp.float32)
            query = query[j * self.per_group : (j + 1) * self.per_group]
            key = self.dk[g : g + 1, :].astype(jnp.float32)
            value = self.dv[g : g + 1, :].astype(jnp.float32)
            score = jnp.sum(query * key, axis=1, keepdims=True)
            new = jnp.maximum(old, score)
            keep = jnp.exp2((old - new) * self.rate)
            own = jnp.exp2((score - new) * self.rate)
            top_sum = keep * part[:, :HEAD_WIDTH] + own * value
            results.append(top_sum / (keep * part[:, HEAD_WIDTH:] + own))
        rows = self.per_piece * self.per_group
        self.nxt[piece * rows : (piece + 1) * rows, :] = jnp.concatenate(results, 0).astype(
            jnp.bfloat16
        )


def ring_kernel(
    n,
    counts,
    offsets,
    pk,
    pv,
    ck,
    cv,
    q_hbm,
    dq_hbm,
    dk_hbm,
    dv_hbm,
    out,
    nxt,
    kv,
    q,
    dq,
    dk,
    dv,
    peak,
    acc,
    sends,
    recvs,
    local,
):
    me = lax.axis_index("ctx")
    lines = n // CHUNK
    z, x, c = me // CHUNK, (me // 2) % 2, me % 2
    last = lines - 1
    half = kv.shape[3]
    own_copies = []
    for p in range(PIECES):
        top = 0
        for i, source in enumerate((pk, pv, ck, cv)):
            rows = source.shape[0]
            own_copies.append(
                pltpu.make_async_copy(
                    source.at[:, p * half : (p + 1) * half],
                    kv.at[p, me, top : top + rows],
                    local.at[4 * p + i],
                )
            )
            top += rows
    for d in own_copies:
        d.start()
    query_copies = [
        pltpu.make_async_copy(source, target, local.at[8 + i])
        for i, (source, target) in enumerate(
            ((q_hbm, q), (dq_hbm, dq), (dk_hbm, dk), (dv_hbm, dv))
        )
    ]
    for d in query_copies:
        d.start()
    to_x = z * CHUNK + (1 - x) * 2 + c
    to_core = z * CHUNK + x * 2 + (1 - c)
    targets = (me + CHUNK, me - CHUNK, to_x, to_core)

    barrier = pltpu.get_barrier_semaphore()

    def greet(target):
        pl.semaphore_signal(
            barrier, inc=1, device_id={"ctx": target}, device_id_type=pl.DeviceIdType.MESH
        )

    greet(to_x)
    greet(to_core)

    @pl.when(z < last)
    def _():
        greet(me + CHUNK)

    @pl.when(z > 0)
    def _():
        greet(me - CHUNK)

    inner = jnp.where((z > 0) & (z < last), 1, 0).astype(jnp.int32)
    pl.semaphore_wait(barrier, 3 + inner)

    def copy(way, source, p):
        return pltpu.make_async_remote_copy(
            src_ref=kv.at[p, source],
            dst_ref=kv.at[p, source],
            send_sem=sends.at[way, source, p],
            recv_sem=recvs.at[source, p],
            device_id={"ctx": targets[way]},
            device_id_type=pl.DeviceIdType.MESH,
        )

    def column(line):
        return line * CHUNK + x * 2 + c

    def spread(line, p, act):
        @pl.when((line <= z) & (z < last))
        def _():
            act(copy(0, column(line), p))

        @pl.when((line >= z) & (z > 0))
        def _():
            act(copy(1, column(line), p))

        act(copy(2, column(line), p))
        act(copy(3, column(line), p))

    def other(line):
        return line * CHUNK + (1 - x) * 2 + c

    def start(d):
        d.start()

    near = jnp.minimum(z, last - z)
    lower = z < lines // 2
    order = []
    for s in range(lines):
        base = s if s >= 2 else (near if s == 0 else 1 - near)
        order.append(jnp.where(lower, base, last - base))

    for p in range(PIECES):
        for d in own_copies[4 * p : 4 * p + 4]:
            d.wait()
        spread(z, p, start)

    body = Body(n, q, dq, dk, dv, counts, offsets, kv, out, nxt, peak, acc)
    body.init()

    def from_column(s, p):
        copy(2, column(order[s]), p).wait_recv()
        spread(order[s], p, start)

    def from_x(s, p):
        copy(3, other(order[s]), p).wait_recv()
        copy(3, other(order[s]), p).start()

    def from_core(s, p):
        for side in range(2):
            copy(2, order[s] * CHUNK + side * 2 + (1 - c), p).wait_recv()

    for p in range(PIECES):
        from_column(1, p)
        from_x(0, p)
    for d in query_copies:
        d.wait()
    for s in range(lines):
        final = s == lines - 1
        masks = body.bias(me, order[s] * CHUNK)
        for p in range(PIECES):
            if s + 2 < lines:
                from_column(s + 2, p)
            from_core(s, p)
            for j in range(body.per_piece):
                body.chunk(p * body.per_piece + j, order[s] * CHUNK, masks, final)
            if s + 1 < lines:
                from_x(s + 1, p)
            if final:
                for j in range(body.per_piece):
                    body.finish(p * body.per_piece + j, me)
                body.finish_step(p)
    for s in range(lines):
        for p in range(PIECES):
            spread(order[s], p, lambda d: d.wait_send())
            copy(3, other(order[s]), p).wait_send()


def local_kernel(n, counts, offsets, kv, q, dq, dk, dv, out, nxt, peak, acc):
    me = lax.axis_index("ctx")
    body = Body(n, q, dq, dk, dv, counts, offsets, kv, out, nxt, peak, acc)
    body.init()
    devices = HEAD_WIDTH // body.prior
    for g in range(body.groups):

        def step(i, carry):
            body.chunk(g, i * CHUNK, body.bias(me, i * CHUNK), False)
            return carry

        def prefix_step(i, carry):
            keys, values = body.prefix_rows(g, i * devices, devices)
            body.update(g, keys, values, None)
            return carry

        lax.fori_loop(0, n // CHUNK, step, 0)
        lax.fori_loop(0, n // devices, prefix_step, 0)
        body.finish(g, me)
    for p in range(PIECES):
        body.finish_step(p)


def body_fn(
    prompt_query,
    prompt_key,
    prompt_value,
    prefix_key_cache,
    prefix_value_cache,
    decoded_query,
    decoded_key,
    decoded_value,
    shard_counts,
    block_offsets,
):
    n = lax.axis_size("ctx")
    rows = prompt_query.shape[0]
    groups = prompt_key.shape[1] // HEAD_WIDTH
    heads = prompt_query.shape[1] // HEAD_WIDTH
    blocks = (prompt_key, prompt_value, prefix_key_cache, prefix_value_cache)
    tables = (shard_counts.T, block_offsets.T)
    half = prompt_key.shape[1] // PIECES
    height = sum(b.shape[0] for b in blocks)
    dq = decoded_query.reshape(heads, HEAD_WIDTH)
    dk = decoded_key.reshape(groups, HEAD_WIDTH)
    dv = decoded_value.reshape(groups, HEAD_WIDTH)
    total = heads // groups * rows + heads // PIECES
    smem = pl.BlockSpec(memory_space=pltpu.SMEM)
    vmem = pl.BlockSpec(memory_space=pltpu.VMEM)
    hbm = pl.BlockSpec(memory_space=pltpu.HBM)
    out_shape = (
        jax.ShapeDtypeStruct(prompt_query.shape, jnp.bfloat16),
        jax.ShapeDtypeStruct((heads, HEAD_WIDTH), jnp.bfloat16),
    )
    state = [
        pltpu.VMEM((groups, total, HEAD_WIDTH), jnp.float32),
        pltpu.VMEM((groups, total, 2 * HEAD_WIDTH), jnp.float32),
    ]
    if n == 4 * CHUNK:
        span, nxt = pl.pallas_call(
            functools.partial(ring_kernel, n),
            out_shape=out_shape,
            in_specs=[smem, smem] + [hbm] * 8,
            out_specs=(vmem, vmem),
            scratch_shapes=[
                pltpu.VMEM((PIECES, n, height, half), jnp.bfloat16),
                pltpu.VMEM(prompt_query.shape, jnp.bfloat16),
                pltpu.VMEM(dq.shape, jnp.bfloat16),
                pltpu.VMEM(dk.shape, jnp.bfloat16),
                pltpu.VMEM(dv.shape, jnp.bfloat16),
                *state,
                pltpu.SemaphoreType.DMA((4, n, PIECES)),
                pltpu.SemaphoreType.DMA((n, PIECES)),
                pltpu.SemaphoreType.DMA((12,)),
            ],
            compiler_params=pltpu.CompilerParams(
                collective_id=0, has_side_effects=True, vmem_limit_bytes=63 * 1024 * 1024
            ),
        )(*tables, *blocks, prompt_query, dq, dk, dv)
    else:
        joined = jnp.concatenate(blocks, axis=0)
        joined = jnp.stack([joined[:, p * half : (p + 1) * half] for p in range(PIECES)], 0)
        gathered = lax.all_gather(joined, "ctx", axis=1)
        span, nxt = pl.pallas_call(
            functools.partial(local_kernel, n),
            out_shape=out_shape,
            in_specs=[smem, smem, vmem, vmem, vmem, vmem, vmem],
            out_specs=(vmem, vmem),
            scratch_shapes=state,
            compiler_params=pltpu.CompilerParams(vmem_limit_bytes=56 * 1024 * 1024),
        )(*tables, gathered, prompt_query, dq, dk, dv)
    return span, nxt.reshape(heads * HEAD_WIDTH)


def solution(mesh):
    both = P(("groups", "ctx"), None)
    in_specs = (
        both,
        both,
        both,
        both,
        both,
        P("groups"),
        P("groups"),
        P("groups"),
        P("groups", None),
        P("groups", None),
    )
    out_specs = (both, P("groups"))
    return jax.shard_map(
        body_fn, mesh=mesh, in_specs=in_specs, out_specs=out_specs, check_vma=False
    )
```

```python
import functools

import jax
import jax.numpy as jnp
from jax import lax
from jax.experimental import pallas as pl
from jax.experimental.pallas import tpu as pltpu
from jax.sharding import PartitionSpec as P

HEAD_WIDTH = 128
PIECES = 2
CHUNK = 4
LOG2E = 1.4426950408889634
FILL = -1e30
FAR = 1 << 29
PLAN = (
    ("further", 0, (0,)),
    ("attend", 0, (0,)),
    ("x", 1, (0,)),
    ("further", 0, (1,)),
    ("attend", 0, (1,)),
    ("x", 1, (1,)),
    ("last", 0, (0,)),
    ("attend", 1, (0,)),
    ("x", 2, (0,)),
    ("last", 0, (1,)),
    ("attend", 1, (1,)),
    ("x", 2, (1,)),
    ("attend", 2, (0,)),
    ("x", 3, (0,)),
    ("attend", 2, (1,)),
    ("x", 3, (1,)),
    ("attend", 3, (0,)),
    ("attend", 3, (1,)),
)


class Body:
    def __init__(self, n, q, dq, dk, dv, counts, offsets, kv, out, nxt, peak, acc):
        self.n, self.q, self.dq, self.dk, self.dv = n, q, dq, dk, dv
        self.counts, self.offsets, self.kv, self.out, self.nxt = counts, offsets, kv, out, nxt
        self.peak, self.acc = peak, acc
        self.rows = q.shape[0]
        self.half = self.rows // 2
        self.prior = (kv.shape[2] - 2 * self.rows) // 2
        self.groups = dk.shape[0]
        self.per_piece = self.groups // PIECES
        self.per_group = q.shape[1] // HEAD_WIDTH // self.groups
        self.tall = self.per_group * self.rows
        self.total = self.tall + self.per_piece * self.per_group
        self.rate = HEAD_WIDTH**-0.5 * LOG2E

    def init(self):
        self.peak[...] = jnp.full(self.peak.shape, FILL, jnp.float32)
        self.acc[...] = jnp.zeros(self.acc.shape, jnp.float32)

    def query_positions(self, me):
        r = lax.broadcasted_iota(jnp.int32, (self.rows, 1), 0)
        second = r >= self.half
        offset = jnp.where(second, r - self.half, r)
        position = offset + jnp.where(second, self.offsets[1, me], self.offsets[0, me])
        live = offset < jnp.where(second, self.counts[1, me], self.counts[0, me])
        return position, live

    def bias(self, me, first):
        width = CHUNK * self.rows
        lane = lax.broadcasted_iota(jnp.int32, (1, width), 1)
        piece = lane // self.half
        offset = lane % self.half
        start = jnp.zeros((1, width), jnp.int32)
        count = jnp.zeros((1, width), jnp.int32)
        for i in range(CHUNK):
            for h in range(2):
                here = piece == 2 * i + h
                start = jnp.where(here, self.offsets[h, first + i], start)
                count = jnp.where(here, self.counts[h, first + i], count)
        position = jnp.where(offset < count, start + offset, FAR)
        own, _ = self.query_positions(me)
        span = jnp.where(position <= own, 0.0, FILL).astype(jnp.float32)
        step = jnp.where(position < FAR, 0.0, FILL).astype(jnp.float32)
        return span, step

    def queries(self, g):
        base = g * self.per_group
        parts = [
            self.q[:, (base + h) * HEAD_WIDTH : (base + h + 1) * HEAD_WIDTH]
            for h in range(self.per_group)
        ]
        piece_rows = self.per_piece * self.per_group
        top = (g // self.per_piece) * piece_rows
        parts.append(self.dq[top : top + piece_rows, :])
        return jnp.concatenate(parts, axis=0)

    def chunk_rows(self, g, first, start):
        j = g % self.per_piece
        block = self.kv[
            g // self.per_piece,
            pl.ds(first, CHUNK),
            start : start + self.rows,
            j * HEAD_WIDTH : (j + 1) * HEAD_WIDTH,
        ]
        return block.reshape(CHUNK * self.rows, HEAD_WIDTH)

    def prefix_rows(self, g, first, devices):
        j = g % self.per_piece
        block = self.kv[
            g // self.per_piece,
            pl.ds(first, devices),
            2 * self.rows :,
            j * HEAD_WIDTH : (j + 1) * HEAD_WIDTH,
        ].astype(jnp.float32)
        flat = (devices * self.prior, HEAD_WIDTH)
        keys = block[:, : self.prior].reshape(flat).astype(jnp.bfloat16)
        values = block[:, self.prior :].reshape(flat).astype(jnp.bfloat16)
        return keys, values

    def update(self, g, keys, values, masks):
        scores = lax.dot_general(
            self.queries(g), keys, (((1,), (1,)), ((), ())), preferred_element_type=jnp.float32
        )
        if masks is not None:
            span, step = masks
            width = span.shape[1]
            extra = scores.shape[1] - width
            if extra:
                span = jnp.concatenate([span, jnp.zeros((span.shape[0], extra), jnp.float32)], 1)
                step = jnp.concatenate([step, jnp.zeros((1, extra), jnp.float32)], 1)
            low = jnp.broadcast_to(step, (self.total - self.tall, step.shape[1]))
            scores = scores + jnp.concatenate([span] * self.per_group + [low], 0)
        old = self.peak[g]
        new = jnp.maximum(old, jnp.max(scores, axis=1, keepdims=True))
        weights = jnp.exp2((scores - new[:, :1]) * self.rate).astype(jnp.bfloat16)
        wide = jnp.concatenate([values, jnp.ones(values.shape, jnp.bfloat16)], 1)
        summed = jnp.dot(weights, wide, preferred_element_type=jnp.float32)
        scale = jnp.exp2((old - new) * self.rate)
        self.acc[g] = self.acc[g] * jnp.concatenate([scale, scale], 1) + summed
        self.peak[g] = new

    def chunk(self, g, first, masks, prefix):
        keys = self.chunk_rows(g, first, 0)
        values = self.chunk_rows(g, first, self.rows)
        if prefix:
            more_keys, more_values = self.prefix_rows(g, 0, self.n)
            keys = jnp.concatenate([keys, more_keys], 0)
            values = jnp.concatenate([values, more_values], 0)
        self.update(g, keys, values, masks)

    def finish(self, g, me):
        _, live = self.query_positions(me)
        base = g * self.per_group
        for h in range(self.per_group):
            part = self.acc[g, h * self.rows : (h + 1) * self.rows, :]
            result = part[:, :HEAD_WIDTH] / part[:, HEAD_WIDTH:]
            result = jnp.where(live, result, 0.0).astype(jnp.bfloat16)
            self.out[:, (base + h) * HEAD_WIDTH : (base + h + 1) * HEAD_WIDTH] = result

    def finish_step(self, piece):
        results = []
        for j in range(self.per_piece):
            g = piece * self.per_piece + j
            top = self.tall + j * self.per_group
            part = self.acc[g, top : top + self.per_group, :]
            old = self.peak[g, top : top + self.per_group, :]
            rows = self.per_piece * self.per_group
            query = self.dq[piece * rows : (piece + 1) * rows, :].astype(jnp.float32)
            query = query[j * self.per_group : (j + 1) * self.per_group]
            key = self.dk[g : g + 1, :].astype(jnp.float32)
            value = self.dv[g : g + 1, :].astype(jnp.float32)
            score = jnp.sum(query * key, axis=1, keepdims=True)
            new = jnp.maximum(old, score)
            keep = jnp.exp2((old - new) * self.rate)
            own = jnp.exp2((score - new) * self.rate)
            top_sum = keep * part[:, :HEAD_WIDTH] + own * value
            results.append(top_sum / (keep * part[:, HEAD_WIDTH:] + own))
        rows = self.per_piece * self.per_group
        self.nxt[piece * rows : (piece + 1) * rows, :] = jnp.concatenate(results, 0).astype(
            jnp.bfloat16
        )


def ring_kernel(
    n,
    counts,
    offsets,
    pk,
    pv,
    ck,
    cv,
    q_hbm,
    dq_hbm,
    dk_hbm,
    dv_hbm,
    out,
    nxt,
    kv,
    q,
    dq,
    dk,
    dv,
    peak,
    acc,
    spans,
    steps,
    sends,
    recvs,
    local,
):
    me = lax.axis_index("ctx")
    lines = n // CHUNK
    z, x, c = me // CHUNK, (me // 2) % 2, me % 2
    last = lines - 1
    half = kv.shape[3]
    own_copies = []
    for p in range(PIECES):
        top = 0
        for i, source in enumerate((pk, pv, ck, cv)):
            rows = source.shape[0]
            own_copies.append(
                pltpu.make_async_copy(
                    source.at[:, p * half : (p + 1) * half],
                    kv.at[p, me, top : top + rows],
                    local.at[4 * p + i],
                )
            )
            top += rows
    for d in own_copies:
        d.start()
    query_copies = [
        pltpu.make_async_copy(source, target, local.at[4 * PIECES + i])
        for i, (source, target) in enumerate(
            ((q_hbm, q), (dq_hbm, dq), (dk_hbm, dk), (dv_hbm, dv))
        )
    ]
    for d in query_copies:
        d.start()
    to_x = z * CHUNK + (1 - x) * 2 + c
    to_core = z * CHUNK + x * 2 + (1 - c)
    targets = (me + CHUNK, me - CHUNK, to_x, to_core)

    barrier = pltpu.get_barrier_semaphore()

    def greet(target):
        pl.semaphore_signal(
            barrier, inc=1, device_id={"ctx": target}, device_id_type=pl.DeviceIdType.MESH
        )

    greet(to_x)
    greet(to_core)

    @pl.when(z < last)
    def _():
        greet(me + CHUNK)

    @pl.when(z > 0)
    def _():
        greet(me - CHUNK)

    inner = jnp.where((z > 0) & (z < last), 1, 0).astype(jnp.int32)
    pl.semaphore_wait(barrier, 3 + inner)

    def copy(way, source, p):
        return pltpu.make_async_remote_copy(
            src_ref=kv.at[p, source],
            dst_ref=kv.at[p, source],
            send_sem=sends.at[way, source, p],
            recv_sem=recvs.at[source, p],
            device_id={"ctx": targets[way]},
            device_id_type=pl.DeviceIdType.MESH,
        )

    def column(line):
        return line * CHUNK + x * 2 + c

    def along(line, p, act):
        @pl.when((line <= z) & (z < last))
        def _():
            act(copy(0, column(line), p))

        @pl.when((line >= z) & (z > 0))
        def _():
            act(copy(1, column(line), p))

    def across(line, p, act):
        act(copy(2, column(line), p))
        act(copy(3, column(line), p))

    def spread(line, p, act):
        along(line, p, act)
        across(line, p, act)

    def other(line):
        return line * CHUNK + (1 - x) * 2 + c

    def start(d):
        d.start()

    near = jnp.minimum(z, last - z)
    lower = z < lines // 2
    order = []
    for s in range(lines):
        base = s if s >= 2 else (near if s == 0 else 1 - near)
        order.append(jnp.where(lower, base, last - base))

    for p in range(PIECES):
        for d in own_copies[4 * p : 4 * p + 4]:
            d.wait()
        spread(z, p, start)

    body = Body(n, q, dq, dk, dv, counts, offsets, kv, out, nxt, peak, acc)

    def arrived(line, p):
        copy(2, column(line), p).wait_recv()

    def from_column(line, p):
        arrived(line, p)
        spread(line, p, start)

    def from_x(s, p):
        copy(3, other(order[s]), p).wait_recv()
        copy(3, other(order[s]), p).start()

    def from_core(s, p):
        for side in range(2):
            copy(2, order[s] * CHUNK + side * 2 + (1 - c), p).wait_recv()

    def attend(s, pieces):
        for p in pieces:
            from_core(s, p)
        masks = (spans[s], steps[s])
        for p in pieces:
            for j in range(body.per_piece):
                body.chunk(p * body.per_piece + j, order[s] * CHUNK, masks, s == lines - 1)
        if s == lines - 1:
            for p in pieces:
                for j in range(body.per_piece):
                    body.finish(p * body.per_piece + j, me)
                body.finish_step(p)

    def only(condition, act, *args):
        @pl.when(condition)
        def _():
            act(*args)

    inside = near == 1
    outside = near == 0
    for p in range(PIECES):
        from_column(order[1], p)

        @pl.when(inside)
        def _():
            arrived(order[2], p)
            along(order[2], p, start)

        from_x(0, p)
        if p == 0:
            for d in query_copies:
                d.wait()
            body.init()
            for s in range(lines):
                spans[s], steps[s] = body.bias(me, order[s] * CHUNK)

    @pl.when(inside)
    def _():
        for p in range(PIECES):
            across(order[2], p, start)

    further = jnp.where(inside, order[3], order[2])
    for kind, s, pieces in PLAN:
        if kind == "attend":
            attend(s, pieces)
        for p in pieces:
            if kind == "further":
                from_column(further, p)
            if kind == "last":
                only(outside, from_column, order[lines - 1], p)
            if kind == "x":
                from_x(s, p)
    for s in range(lines):
        for p in range(PIECES):
            spread(order[s], p, lambda d: d.wait_send())
            copy(3, other(order[s]), p).wait_send()


def local_kernel(n, counts, offsets, kv, q, dq, dk, dv, out, nxt, peak, acc):
    me = lax.axis_index("ctx")
    body = Body(n, q, dq, dk, dv, counts, offsets, kv, out, nxt, peak, acc)
    body.init()
    devices = HEAD_WIDTH // body.prior
    for g in range(body.groups):

        def step(i, carry):
            body.chunk(g, i * CHUNK, body.bias(me, i * CHUNK), False)
            return carry

        def prefix_step(i, carry):
            keys, values = body.prefix_rows(g, i * devices, devices)
            body.update(g, keys, values, None)
            return carry

        lax.fori_loop(0, n // CHUNK, step, 0)
        lax.fori_loop(0, n // devices, prefix_step, 0)
        body.finish(g, me)
    for p in range(PIECES):
        body.finish_step(p)


def body_fn(
    prompt_query,
    prompt_key,
    prompt_value,
    prefix_key_cache,
    prefix_value_cache,
    decoded_query,
    decoded_key,
    decoded_value,
    shard_counts,
    block_offsets,
):
    n = lax.axis_size("ctx")
    rows = prompt_query.shape[0]
    groups = prompt_key.shape[1] // HEAD_WIDTH
    heads = prompt_query.shape[1] // HEAD_WIDTH
    blocks = (prompt_key, prompt_value, prefix_key_cache, prefix_value_cache)
    tables = (shard_counts.T, block_offsets.T)
    half = prompt_key.shape[1] // PIECES
    height = sum(b.shape[0] for b in blocks)
    dq = decoded_query.reshape(heads, HEAD_WIDTH)
    dk = decoded_key.reshape(groups, HEAD_WIDTH)
    dv = decoded_value.reshape(groups, HEAD_WIDTH)
    total = heads // groups * rows + heads // PIECES
    smem = pl.BlockSpec(memory_space=pltpu.SMEM)
    vmem = pl.BlockSpec(memory_space=pltpu.VMEM)
    hbm = pl.BlockSpec(memory_space=pltpu.HBM)
    out_shape = (
        jax.ShapeDtypeStruct(prompt_query.shape, jnp.bfloat16),
        jax.ShapeDtypeStruct((heads, HEAD_WIDTH), jnp.bfloat16),
    )
    state = [
        pltpu.VMEM((groups, total, HEAD_WIDTH), jnp.float32),
        pltpu.VMEM((groups, total, 2 * HEAD_WIDTH), jnp.float32),
    ]
    if n == 4 * CHUNK:
        span, nxt = pl.pallas_call(
            functools.partial(ring_kernel, n),
            out_shape=out_shape,
            in_specs=[smem, smem] + [hbm] * 8,
            out_specs=(vmem, vmem),
            scratch_shapes=[
                pltpu.VMEM((PIECES, n, height, half), jnp.bfloat16),
                pltpu.VMEM(prompt_query.shape, jnp.bfloat16),
                pltpu.VMEM(dq.shape, jnp.bfloat16),
                pltpu.VMEM(dk.shape, jnp.bfloat16),
                pltpu.VMEM(dv.shape, jnp.bfloat16),
                *state,
                pltpu.VMEM((n // CHUNK, rows, CHUNK * rows), jnp.float32),
                pltpu.VMEM((n // CHUNK, 1, CHUNK * rows), jnp.float32),
                pltpu.SemaphoreType.DMA((4, n, PIECES)),
                pltpu.SemaphoreType.DMA((n, PIECES)),
                pltpu.SemaphoreType.DMA((4 * PIECES + 4,)),
            ],
            compiler_params=pltpu.CompilerParams(
                collective_id=0, has_side_effects=True, vmem_limit_bytes=63 * 1024 * 1024
            ),
        )(*tables, *blocks, prompt_query, dq, dk, dv)
    else:
        joined = jnp.concatenate(blocks, axis=0)
        joined = jnp.stack([joined[:, p * half : (p + 1) * half] for p in range(PIECES)], 0)
        gathered = lax.all_gather(joined, "ctx", axis=1)
        span, nxt = pl.pallas_call(
            functools.partial(local_kernel, n),
            out_shape=out_shape,
            in_specs=[smem, smem, vmem, vmem, vmem, vmem, vmem],
            out_specs=(vmem, vmem),
            scratch_shapes=state,
            compiler_params=pltpu.CompilerParams(vmem_limit_bytes=56 * 1024 * 1024),
        )(*tables, gathered, prompt_query, dq, dk, dv)
    return span, nxt.reshape(heads * HEAD_WIDTH)


def solution(mesh):
    both = P(("groups", "ctx"), None)
    in_specs = (
        both,
        both,
        both,
        both,
        both,
        P("groups"),
        P("groups"),
        P("groups"),
        P("groups", None),
        P("groups", None),
    )
    out_specs = (both, P("groups"))
    return jax.shard_map(
        body_fn, mesh=mesh, in_specs=in_specs, out_specs=out_specs, check_vma=False
    )
```

```python
import functools

import jax
import jax.numpy as jnp
from jax import lax
from jax.experimental import pallas as pl
from jax.experimental.pallas import tpu as pltpu
from jax.sharding import PartitionSpec as P

HEAD_WIDTH = 128
PIECES = 2
CHUNK = 4
LOG2E = 1.4426950408889634
FILL = -1e30
FAR = 1 << 29
PLAN = (
    ("further", 0, (0,)),
    ("attend", 0, (0,)),
    ("x", 1, (0,)),
    ("further", 0, (1,)),
    ("attend", 0, (1,)),
    ("x", 1, (1,)),
    ("last", 0, (0,)),
    ("attend", 1, (0,)),
    ("x", 2, (0,)),
    ("last", 0, (1,)),
    ("attend", 1, (1,)),
    ("x", 2, (1,)),
    ("attend", 2, (0,)),
    ("x", 3, (0,)),
    ("attend", 2, (1,)),
    ("x", 3, (1,)),
    ("attend", 3, (0,)),
    ("attend", 3, (1,)),
)


class Body:
    def __init__(self, n, q, dq, dk, dv, counts, offsets, kv, out, nxt, peak, acc):
        self.n, self.q, self.dq, self.dk, self.dv = n, q, dq, dk, dv
        self.counts, self.offsets, self.kv, self.out, self.nxt = counts, offsets, kv, out, nxt
        self.peak, self.acc = peak, acc
        self.rows = q.shape[0]
        self.half = self.rows // 2
        self.prior = (kv.shape[2] - 2 * self.rows) // 2
        self.groups = dk.shape[0]
        self.per_piece = self.groups // PIECES
        self.per_group = q.shape[1] // HEAD_WIDTH // self.groups
        self.tall = self.per_group * self.rows
        self.total = self.tall + self.per_piece * self.per_group
        self.rate = HEAD_WIDTH**-0.5 * LOG2E

    def init(self):
        self.peak[...] = jnp.full(self.peak.shape, FILL, jnp.float32)
        self.acc[...] = jnp.zeros(self.acc.shape, jnp.float32)

    def query_positions(self, me):
        r = lax.broadcasted_iota(jnp.int32, (self.rows, 1), 0)
        second = r >= self.half
        offset = jnp.where(second, r - self.half, r)
        position = offset + jnp.where(second, self.offsets[1, me], self.offsets[0, me])
        live = offset < jnp.where(second, self.counts[1, me], self.counts[0, me])
        return position, live

    def bias(self, me, first):
        width = CHUNK * self.rows
        lane = lax.broadcasted_iota(jnp.int32, (1, width), 1)
        piece = lane // self.half
        offset = lane % self.half
        start = jnp.zeros((1, width), jnp.int32)
        count = jnp.zeros((1, width), jnp.int32)
        for i in range(CHUNK):
            for h in range(2):
                here = piece == 2 * i + h
                start = jnp.where(here, self.offsets[h, first + i], start)
                count = jnp.where(here, self.counts[h, first + i], count)
        position = jnp.where(offset < count, start + offset, FAR)
        own, _ = self.query_positions(me)
        span = jnp.where(position <= own, 0.0, FILL).astype(jnp.float32)
        step = jnp.where(position < FAR, 0.0, FILL).astype(jnp.float32)
        return span, step

    def queries(self, g):
        base = g * self.per_group
        parts = [
            self.q[:, (base + h) * HEAD_WIDTH : (base + h + 1) * HEAD_WIDTH]
            for h in range(self.per_group)
        ]
        piece_rows = self.per_piece * self.per_group
        top = (g // self.per_piece) * piece_rows
        parts.append(self.dq[top : top + piece_rows, :])
        return jnp.concatenate(parts, axis=0)

    def chunk_rows(self, g, first, start):
        j = g % self.per_piece
        block = self.kv[
            g // self.per_piece,
            pl.ds(first, CHUNK),
            start : start + self.rows,
            j * HEAD_WIDTH : (j + 1) * HEAD_WIDTH,
        ]
        return block.reshape(CHUNK * self.rows, HEAD_WIDTH)

    def prefix_rows(self, g, first, devices):
        j = g % self.per_piece
        block = self.kv[
            g // self.per_piece,
            pl.ds(first, devices),
            2 * self.rows :,
            j * HEAD_WIDTH : (j + 1) * HEAD_WIDTH,
        ].astype(jnp.float32)
        flat = (devices * self.prior, HEAD_WIDTH)
        keys = block[:, : self.prior].reshape(flat).astype(jnp.bfloat16)
        values = block[:, self.prior :].reshape(flat).astype(jnp.bfloat16)
        return keys, values

    def update(self, g, keys, values, masks):
        scores = lax.dot_general(
            self.queries(g), keys, (((1,), (1,)), ((), ())), preferred_element_type=jnp.float32
        )
        if masks is not None:
            span, step = masks
            width = span.shape[1]
            extra = scores.shape[1] - width
            if extra:
                span = jnp.concatenate([span, jnp.zeros((span.shape[0], extra), jnp.float32)], 1)
                step = jnp.concatenate([step, jnp.zeros((1, extra), jnp.float32)], 1)
            low = jnp.broadcast_to(step, (self.total - self.tall, step.shape[1]))
            scores = scores + jnp.concatenate([span] * self.per_group + [low], 0)
        old = self.peak[g]
        new = jnp.maximum(old, jnp.max(scores, axis=1, keepdims=True))
        weights = jnp.exp2((scores - new[:, :1]) * self.rate).astype(jnp.bfloat16)
        wide = jnp.concatenate([values, jnp.ones(values.shape, jnp.bfloat16)], 1)
        summed = jnp.dot(weights, wide, preferred_element_type=jnp.float32)
        scale = jnp.exp2((old - new) * self.rate)
        self.acc[g] = self.acc[g] * jnp.concatenate([scale, scale], 1) + summed
        self.peak[g] = new

    def chunk(self, g, first, masks, prefix):
        keys = self.chunk_rows(g, first, 0)
        values = self.chunk_rows(g, first, self.rows)
        if prefix:
            more_keys, more_values = self.prefix_rows(g, 0, self.n)
            keys = jnp.concatenate([keys, more_keys], 0)
            values = jnp.concatenate([values, more_values], 0)
        self.update(g, keys, values, masks)

    def finish(self, g, me):
        _, live = self.query_positions(me)
        base = g * self.per_group
        for h in range(self.per_group):
            part = self.acc[g, h * self.rows : (h + 1) * self.rows, :]
            result = part[:, :HEAD_WIDTH] / part[:, HEAD_WIDTH:]
            result = jnp.where(live, result, 0.0).astype(jnp.bfloat16)
            self.out[:, (base + h) * HEAD_WIDTH : (base + h + 1) * HEAD_WIDTH] = result

    def finish_step(self, piece):
        results = []
        for j in range(self.per_piece):
            g = piece * self.per_piece + j
            top = self.tall + j * self.per_group
            part = self.acc[g, top : top + self.per_group, :]
            old = self.peak[g, top : top + self.per_group, :]
            rows = self.per_piece * self.per_group
            query = self.dq[piece * rows : (piece + 1) * rows, :].astype(jnp.float32)
            query = query[j * self.per_group : (j + 1) * self.per_group]
            key = self.dk[g : g + 1, :].astype(jnp.float32)
            value = self.dv[g : g + 1, :].astype(jnp.float32)
            score = jnp.sum(query * key, axis=1, keepdims=True)
            new = jnp.maximum(old, score)
            keep = jnp.exp2((old - new) * self.rate)
            own = jnp.exp2((score - new) * self.rate)
            top_sum = keep * part[:, :HEAD_WIDTH] + own * value
            results.append(top_sum / (keep * part[:, HEAD_WIDTH:] + own))
        rows = self.per_piece * self.per_group
        self.nxt[piece * rows : (piece + 1) * rows, :] = jnp.concatenate(results, 0).astype(
            jnp.bfloat16
        )


def ring_kernel(
    n,
    counts,
    offsets,
    pk,
    pv,
    ck,
    cv,
    q_hbm,
    dq_hbm,
    dk_hbm,
    dv_hbm,
    out,
    nxt,
    kv,
    q,
    dq,
    dk,
    dv,
    peak,
    acc,
    spans,
    steps,
    sends,
    recvs,
    local,
):
    me = lax.axis_index("ctx")
    lines = n // CHUNK
    z, x, c = me // CHUNK, (me // 2) % 2, me % 2
    last = lines - 1
    half = kv.shape[3]
    own_copies = []
    for p in range(PIECES):
        top = 0
        for i, source in enumerate((pk, pv, ck, cv)):
            rows = source.shape[0]
            own_copies.append(
                pltpu.make_async_copy(
                    source.at[:, p * half : (p + 1) * half],
                    kv.at[p, me, top : top + rows],
                    local.at[4 * p + i],
                )
            )
            top += rows
    for d in own_copies:
        d.start()
    query_copies = [
        pltpu.make_async_copy(source, target, local.at[4 * PIECES + i])
        for i, (source, target) in enumerate(
            ((q_hbm, q), (dq_hbm, dq), (dk_hbm, dk), (dv_hbm, dv))
        )
    ]
    for d in query_copies:
        d.start()
    to_x = z * CHUNK + (1 - x) * 2 + c
    to_core = z * CHUNK + x * 2 + (1 - c)
    targets = (me + CHUNK, me - CHUNK, to_x, to_core)

    barrier = pltpu.get_barrier_semaphore()

    def greet(target):
        pl.semaphore_signal(
            barrier, inc=1, device_id={"ctx": target}, device_id_type=pl.DeviceIdType.MESH
        )

    greet(to_x)
    greet(to_core)

    @pl.when(z < last)
    def _():
        greet(me + CHUNK)

    @pl.when(z > 0)
    def _():
        greet(me - CHUNK)

    inner = jnp.where((z > 0) & (z < last), 1, 0).astype(jnp.int32)
    pl.semaphore_wait(barrier, 3 + inner)

    def copy(way, source, p):
        return pltpu.make_async_remote_copy(
            src_ref=kv.at[p, source],
            dst_ref=kv.at[p, source],
            send_sem=sends.at[way, source, p],
            recv_sem=recvs.at[source, p],
            device_id={"ctx": targets[way]},
            device_id_type=pl.DeviceIdType.MESH,
        )

    def column(line):
        return line * CHUNK + x * 2 + c

    def along(line, p, act):
        @pl.when((line <= z) & (z < last))
        def _():
            act(copy(0, column(line), p))

        @pl.when((line >= z) & (z > 0))
        def _():
            act(copy(1, column(line), p))

    def across(line, p, act):
        act(copy(2, column(line), p))
        act(copy(3, column(line), p))

    def spread(line, p, act):
        along(line, p, act)
        across(line, p, act)

    def other(line):
        return line * CHUNK + (1 - x) * 2 + c

    def start(d):
        d.start()

    near = jnp.minimum(z, last - z)
    lower = z < lines // 2
    order = []
    for s in range(lines):
        base = s if s >= 2 else (near if s == 0 else 1 - near)
        order.append(jnp.where(lower, base, last - base))

    for p in range(PIECES):
        for d in own_copies[4 * p : 4 * p + 4]:
            d.wait()
        spread(z, p, start)

    body = Body(n, q, dq, dk, dv, counts, offsets, kv, out, nxt, peak, acc)

    def arrived(line, p):
        copy(2, column(line), p).wait_recv()

    def from_column(line, p):
        arrived(line, p)
        spread(line, p, start)

    def from_x(s, p):
        copy(3, other(order[s]), p).wait_recv()
        copy(3, other(order[s]), p).start()

    def from_core(s, p):
        for side in range(2):
            copy(2, order[s] * CHUNK + side * 2 + (1 - c), p).wait_recv()

    def attend(s, pieces):
        for p in pieces:
            from_core(s, p)
        masks = (spans[s], steps[s])
        for p in pieces:
            for j in range(body.per_piece):
                body.chunk(p * body.per_piece + j, order[s] * CHUNK, masks, s == lines - 1)
        if s == lines - 1:
            for p in pieces:
                for j in range(body.per_piece):
                    body.finish(p * body.per_piece + j, me)
                body.finish_step(p)

    def only(condition, act, *args):
        @pl.when(condition)
        def _():
            act(*args)

    inside = near == 1
    outside = near == 0
    body.init()
    for s in range(lines):
        spans[s], steps[s] = body.bias(me, order[s] * CHUNK)
    for p in range(PIECES):
        from_column(order[1], p)

        @pl.when(inside)
        def _():
            arrived(order[2], p)
            along(order[2], p, start)

        from_x(0, p)
        if p == 0:
            for d in query_copies:
                d.wait()

    @pl.when(inside)
    def _():
        for p in range(PIECES):
            across(order[2], p, start)

    further = jnp.where(inside, order[3], order[2])
    for kind, s, pieces in PLAN:
        if kind == "attend":
            attend(s, pieces)
        for p in pieces:
            if kind == "further":
                from_column(further, p)
            if kind == "last":
                only(outside, from_column, order[lines - 1], p)
            if kind == "x":
                from_x(s, p)
    for s in range(lines):
        for p in range(PIECES):
            spread(order[s], p, lambda d: d.wait_send())
            copy(3, other(order[s]), p).wait_send()


def local_kernel(n, counts, offsets, kv, q, dq, dk, dv, out, nxt, peak, acc):
    me = lax.axis_index("ctx")
    body = Body(n, q, dq, dk, dv, counts, offsets, kv, out, nxt, peak, acc)
    body.init()
    devices = HEAD_WIDTH // body.prior
    for g in range(body.groups):

        def step(i, carry):
            body.chunk(g, i * CHUNK, body.bias(me, i * CHUNK), False)
            return carry

        def prefix_step(i, carry):
            keys, values = body.prefix_rows(g, i * devices, devices)
            body.update(g, keys, values, None)
            return carry

        lax.fori_loop(0, n // CHUNK, step, 0)
        lax.fori_loop(0, n // devices, prefix_step, 0)
        body.finish(g, me)
    for p in range(PIECES):
        body.finish_step(p)


def body_fn(
    prompt_query,
    prompt_key,
    prompt_value,
    prefix_key_cache,
    prefix_value_cache,
    decoded_query,
    decoded_key,
    decoded_value,
    shard_counts,
    block_offsets,
):
    n = lax.axis_size("ctx")
    rows = prompt_query.shape[0]
    groups = prompt_key.shape[1] // HEAD_WIDTH
    heads = prompt_query.shape[1] // HEAD_WIDTH
    blocks = (prompt_key, prompt_value, prefix_key_cache, prefix_value_cache)
    tables = (shard_counts.T, block_offsets.T)
    half = prompt_key.shape[1] // PIECES
    height = sum(b.shape[0] for b in blocks)
    dq = decoded_query.reshape(heads, HEAD_WIDTH)
    dk = decoded_key.reshape(groups, HEAD_WIDTH)
    dv = decoded_value.reshape(groups, HEAD_WIDTH)
    total = heads // groups * rows + heads // PIECES
    smem = pl.BlockSpec(memory_space=pltpu.SMEM)
    vmem = pl.BlockSpec(memory_space=pltpu.VMEM)
    hbm = pl.BlockSpec(memory_space=pltpu.HBM)
    out_shape = (
        jax.ShapeDtypeStruct(prompt_query.shape, jnp.bfloat16),
        jax.ShapeDtypeStruct((heads, HEAD_WIDTH), jnp.bfloat16),
    )
    state = [
        pltpu.VMEM((groups, total, HEAD_WIDTH), jnp.float32),
        pltpu.VMEM((groups, total, 2 * HEAD_WIDTH), jnp.float32),
    ]
    if n == 4 * CHUNK:
        span, nxt = pl.pallas_call(
            functools.partial(ring_kernel, n),
            out_shape=out_shape,
            in_specs=[smem, smem] + [hbm] * 8,
            out_specs=(vmem, vmem),
            scratch_shapes=[
                pltpu.VMEM((PIECES, n, height, half), jnp.bfloat16),
                pltpu.VMEM(prompt_query.shape, jnp.bfloat16),
                pltpu.VMEM(dq.shape, jnp.bfloat16),
                pltpu.VMEM(dk.shape, jnp.bfloat16),
                pltpu.VMEM(dv.shape, jnp.bfloat16),
                *state,
                pltpu.VMEM((n // CHUNK, rows, CHUNK * rows), jnp.float32),
                pltpu.VMEM((n // CHUNK, 1, CHUNK * rows), jnp.float32),
                pltpu.SemaphoreType.DMA((4, n, PIECES)),
                pltpu.SemaphoreType.DMA((n, PIECES)),
                pltpu.SemaphoreType.DMA((4 * PIECES + 4,)),
            ],
            compiler_params=pltpu.CompilerParams(
                collective_id=0, has_side_effects=True, vmem_limit_bytes=63 * 1024 * 1024
            ),
        )(*tables, *blocks, prompt_query, dq, dk, dv)
    else:
        joined = jnp.concatenate(blocks, axis=0)
        joined = jnp.stack([joined[:, p * half : (p + 1) * half] for p in range(PIECES)], 0)
        gathered = lax.all_gather(joined, "ctx", axis=1)
        span, nxt = pl.pallas_call(
            functools.partial(local_kernel, n),
            out_shape=out_shape,
            in_specs=[smem, smem, vmem, vmem, vmem, vmem, vmem],
            out_specs=(vmem, vmem),
            scratch_shapes=state,
            compiler_params=pltpu.CompilerParams(vmem_limit_bytes=56 * 1024 * 1024),
        )(*tables, gathered, prompt_query, dq, dk, dv)
    return span, nxt.reshape(heads * HEAD_WIDTH)


def solution(mesh):
    both = P(("groups", "ctx"), None)
    in_specs = (
        both,
        both,
        both,
        both,
        both,
        P("groups"),
        P("groups"),
        P("groups"),
        P("groups", None),
        P("groups", None),
    )
    out_specs = (both, P("groups"))
    return jax.shard_map(
        body_fn, mesh=mesh, in_specs=in_specs, out_specs=out_specs, check_vma=False
    )
```
